32 devices in a mesh: tok: 16 (over z, y, x), head: 2 (over core).
Axes of the slice: x: 2, y: 2, z: 4, core: 2. Of those that a mesh axis runs over, the one named last changes fastest.
Arguments:
- text_queries: bfloat16 [256, 8192], P('tok', 'head'), may hold values from -6 to 6
- text_grads: bfloat16 [256, 8192], P('tok', 'head'), may hold values from -6 to 6
- vision_keys: bfloat16 [8192, 1024], P('tok', 'head'), may hold values from -6 to 6
- video_value_rows: bfloat16 [8192, 1024], P('tok', 'head'), may hold values from -6 to 6
- vision: bfloat16 [8192, 4096], P('tok'), may hold values from -6 to 6
- lengths: int32 [8], replicated, may hold values from 16 to 48, as said below
- frame_range: int32 [8, 2], replicated, may hold values from 0 to 64, as said below
Outputs:
- query_grad: bfloat16 [256, 8192], P(None, 'head')
- key_weight_grad: float32 [4096, 1024], P('tok', 'head')
- value_weight_grad: float32 [4096, 1024], P('tok', 'head')
The draws below stay inside these ranges and needn't reach their ends.
Inputs may be any that keep to these rules, and one draw needn't show every extreme that they name: Each segment holds at least one row; the lengths sum to 256. `frame_range`: each segment's range covers 64 // 4 frames or more, first entry below the second.
All inputs are finite; a program needn't handle non-finite values.
Results may differ from the reference program's by a relative error of at most 0.0073.
Values may be sent and summed in bfloat16 or wider, within the bound.
A program may use at most 128 MiB of HBM per device.

```python
import jax
import jax.numpy as jnp
from jax import lax

QUERY_HEADS = 64
KEY_VALUE_HEADS = 8
HEAD_WIDTH = 128
DW = 4096
TQ = 256
TEXT_SEGMENTS = 8
FRAME_TOK = 128
FRAMES = 64
VIDEO_TOKENS = 8192


def layout(key):
    base_key = jax.random.fold_in(key, 7001)
    base_rows = TQ // TEXT_SEGMENTS
    spread = base_rows // 4
    shifts = jax.random.randint(jax.random.fold_in(base_key, 1), (TEXT_SEGMENTS,), -spread, spread + 1)
    segment_ids = jnp.arange(TEXT_SEGMENTS, dtype=jnp.int32)
    shifts = jnp.where(segment_ids <= 1, spread, shifts)
    shifts = jnp.where(segment_ids == 2, -spread, shifts)
    shifts = jnp.where(segment_ids == TEXT_SEGMENTS - 1, -spread, shifts)
    seg_rows = base_rows + shifts - jnp.roll(shifts, 1)
    fewest = FRAMES // 4
    first_frame = jax.random.randint(jax.random.fold_in(base_key, 2), (TEXT_SEGMENTS,), 0, FRAMES - fewest + 1)
    first_frame = jnp.where(segment_ids == 0, 0, first_frame)
    extension = jax.random.randint(jax.random.fold_in(base_key, 3), (TEXT_SEGMENTS,), 0, FRAMES - fewest - first_frame + 1)
    extension = jnp.where(segment_ids == 1, FRAMES - fewest - first_frame, extension)
    end_frame = first_frame + fewest + extension
    ranges = jnp.stack([first_frame, end_frame], axis=1)
    return (seg_rows.astype(jnp.int32), ranges.astype(jnp.int32))


def paired(key):
    paired_key = jax.random.fold_in(key, 7002)
    query_rows = jnp.clip(1.5 * jax.random.normal(jax.random.fold_in(paired_key, 5), (TQ, QUERY_HEADS * HEAD_WIDTH), jnp.float32), -5.5, 5.5)
    key_row_block = jnp.clip(1.5 * jax.random.normal(jax.random.fold_in(paired_key, 6), (VIDEO_TOKENS, KEY_VALUE_HEADS * HEAD_WIDTH), jnp.float32), -5.5, 5.5)
    return (query_rows, key_row_block)


def draw_lengths(key, part):
    return layout(key)[0]


def draw_frame_range(key, part):
    return layout(key)[1]


def draw_text_queries(key, part):
    return paired(key)[0].astype(jnp.bfloat16)


def draw_vision_keys(key, part):
    return paired(key)[1].astype(jnp.bfloat16)


def spiked(drawn, rng, source, target, parts, factor):
    owner, partner = [(jnp.arange(drawn.shape[dim]) // (drawn.shape[dim] // parts)).reshape([-1 if axis == dim else 1 for axis in range(drawn.ndim)]) for dim in (source, target)]
    chosen = jax.random.permutation(rng, parts)[partner]
    strong = (owner == chosen) | (owner == (partner + parts // 2) % parts)
    return jnp.where(strong, factor * drawn, drawn)


def steps_of(stream_key, dims, pieces, least, high):
    def one(dim, parts):
        heights = jax.random.uniform(jax.random.fold_in(jax.random.fold_in(stream_key, 6), dim), (parts,), jnp.float32, least / len(pieces), high / len(pieces))
        return jnp.repeat(jnp.exp(heights), dims[dim] // parts).reshape((-1,) + (1,) * (len(dims) - dim - 1))

    factor_of = one(*pieces[0])
    for cut in pieces[1:]:
        factor_of = factor_of * one(*cut)
    return factor_of


def noise(key, shape, scale, limit, shards=(), kind=jnp.bfloat16):
    factor_of = steps_of(key, shape, shards, -0.22, 0.18) if shards else 1.0
    drawn = jax.random.normal(key, shape, jnp.float32) * scale * factor_of
    return jnp.minimum(jnp.maximum(drawn, -limit), limit).astype(kind)


def noise_with(key, extent, scale, bound, shards, heavy, held_as=jnp.bfloat16):
    drawn = scale * jax.random.normal(key, extent, jnp.float32)
    if shards:
        drawn = drawn * steps_of(key, extent, shards, -0.22, 0.18)
    return jnp.clip(spiked(drawn, jax.random.fold_in(key, 3), *heavy), -bound, bound).astype(held_as)


def setup_inputs(seed: int = 0) -> dict:
    splits = jax.random.split(jax.random.key(seed), 8)
    return {
        "text_queries": draw_text_queries(jax.random.fold_in(splits[7], 71), 0),
        "text_grads": noise(splits[1], (TQ, QUERY_HEADS * HEAD_WIDTH), 1.0, 6.0, ((0, 16), (1, 2))),
        "vision_keys": draw_vision_keys(jax.random.fold_in(splits[7], 71), 0),
        "video_value_rows": noise(splits[3], (VIDEO_TOKENS, KEY_VALUE_HEADS * HEAD_WIDTH), 1.0, 6.0, ((0, 16), (1, 2))),
        "vision": noise_with(splits[4], (VIDEO_TOKENS, DW), 1.0, 6.0, ((0, 16),), (0, 1, 16, 2.0)),
        "lengths": draw_lengths(jax.random.fold_in(splits[7], 71), 0),
        "frame_range": draw_frame_range(jax.random.fold_in(splits[7], 71), 0),
    }


NEG_FILL = -1e30


def row_bounds(lengths, frame_range):
    row_ids = jnp.arange(TQ, dtype=jnp.int32)
    segment_ends = jnp.cumsum(lengths).astype(jnp.int32)
    segment = jnp.sum((row_ids[:, None] >= segment_ends[None, :]).astype(jnp.int32), axis=1)
    segment_pick = (segment[:, None] == jnp.arange(TEXT_SEGMENTS, dtype=jnp.int32)[None, :]).astype(jnp.int32)
    first_frame = jnp.sum(segment_pick * frame_range[None, :, 0], axis=1)
    end_frame = jnp.sum(segment_pick * frame_range[None, :, 1], axis=1)
    return first_frame, end_frame


def reference(text_queries, text_grads, vision_keys, video_value_rows, vision, lengths, frame_range):
    group_width = QUERY_HEADS // KEY_VALUE_HEADS
    score_scale = HEAD_WIDTH ** -0.5
    first_frame, end_frame = row_bounds(lengths, frame_range)
    frames = jnp.arange(VIDEO_TOKENS, dtype=jnp.int32) // FRAME_TOK
    allowed = (frames[None, :] >= first_frame[:, None]) & (frames[None, :] < end_frame[:, None])

    def head_gradient_list(kv_head):
        k_head = lax.dynamic_slice_in_dim(vision_keys, kv_head * HEAD_WIDTH, HEAD_WIDTH, 1)
        v_head = lax.dynamic_slice_in_dim(video_value_rows, kv_head * HEAD_WIDTH, HEAD_WIDTH, 1)

        def query_head(running, member):
            q_index = kv_head * group_width + member
            q_one = lax.dynamic_slice_in_dim(text_queries, q_index * HEAD_WIDTH, HEAD_WIDTH, 1)
            g_one = lax.dynamic_slice_in_dim(text_grads, q_index * HEAD_WIDTH, HEAD_WIDTH, 1)
            scores = jnp.dot(q_one, k_head.T, preferred_element_type=jnp.float32) * score_scale
            row_top = jnp.max(jnp.where(allowed, scores, NEG_FILL), axis=1, keepdims=True)
            exp_terms = jnp.where(allowed, jnp.exp(scores - row_top), 0.0)
            row_total = jnp.sum(exp_terms, axis=1, keepdims=True)
            attn_probs = exp_terms / row_total
            dprobs = jnp.dot(g_one, v_head.T, preferred_element_type=jnp.float32)
            row_delta = jnp.sum(attn_probs * dprobs, axis=1, keepdims=True)
            dscore = (attn_probs * (dprobs - row_delta)).astype(jnp.bfloat16)
            key_sum = running[0] + jnp.dot(dscore.T, q_one, preferred_element_type=jnp.float32)
            value_sum = running[1] + jnp.dot(attn_probs.astype(jnp.bfloat16).T, g_one, preferred_element_type=jnp.float32)
            dq_part = score_scale * jnp.dot(dscore, k_head, preferred_element_type=jnp.float32)
            return (key_sum, value_sum), dq_part

        zero_acc = jnp.zeros((VIDEO_TOKENS, HEAD_WIDTH), jnp.float32)
        sums, dq_parts = lax.scan(query_head, (zero_acc, zero_acc), jnp.arange(group_width, dtype=jnp.int32))
        return dq_parts, (score_scale * sums[0]).astype(jnp.bfloat16), sums[1].astype(jnp.bfloat16)

    query_gradient_total, key_gradient_total, value_gradient_total = lax.map(head_gradient_list, jnp.arange(KEY_VALUE_HEADS, dtype=jnp.int32))
    query_grad = query_gradient_total.transpose(2, 0, 1, 3).reshape(TQ, QUERY_HEADS * HEAD_WIDTH).astype(jnp.bfloat16)
    key_gradient_flat = key_gradient_total.transpose(1, 0, 2).reshape(VIDEO_TOKENS, KEY_VALUE_HEADS * HEAD_WIDTH)
    value_gradient_flat = value_gradient_total.transpose(1, 0, 2).reshape(VIDEO_TOKENS, KEY_VALUE_HEADS * HEAD_WIDTH)
    key_weight_grad = jnp.dot(vision.T, key_gradient_flat, preferred_element_type=jnp.float32)
    value_weight_grad = jnp.dot(vision.T, value_gradient_flat, preferred_element_type=jnp.float32)
    return query_grad, key_weight_grad, value_weight_grad
```

```python
import functools

import jax
import jax.numpy as jnp
from jax import lax
from jax.experimental import pallas as pl
from jax.experimental.pallas import tpu as pltpu
from jax.sharding import PartitionSpec as P

HEAD_WIDTH = 128
FRAME_DEV = 4
NEG_FILL = -1e30
NT = (((1,), (1,)), ((), ()))
TN = (((0,), (0,)), ((), ()))
F32 = jnp.float32
BF16 = jnp.bfloat16


def dot(a, b, dims=(((1,), (0,)), ((), ()))):
    return lax.dot_general(a, b, dims, preferred_element_type=F32)


def kernel(cfg, q_in, g_in, k_in, v_in, x_in, bounds, q_out, kw_out, vw_out,
           qb, gb, kb, vb, vis, ebuf, dpb, stat, stin, coef, kv, dqt, dqs, dqin, dqall, part, rsb,
           loc, qs, qr, gs, gr, ks, kr, vs, vr, xs, xr, ss, sr, kvs, kvr, ds, dr, as_, ar, ys, yr, rs, rr):
    T, G, NZ = cfg["T"], cfg["G"], cfg["NZ"]
    blk, rows, NK, NR, FR = cfg["blk"], cfg["rows"], cfg["NK"], cfg["NR"], cfg["FR"]
    W, NV, FB = cfg["W"], cfg["NV"], cfg["FB"]
    RB = cfg["RB"]
    scale = HEAD_WIDTH ** (-0.5)
    me = lax.axis_index("tok")
    z, j0 = me // G, me % G

    def remote(src, dst, s, r, peer):
        return pltpu.make_async_remote_copy(
            src_ref=src, dst_ref=dst, send_sem=s, recv_sem=r,
            device_id={"tok": peer}, device_id_type=pl.DeviceIdType.MESH)

    def m128(i, n):
        return pl.ds(pl.multiple_of(i * n, n), n)

    barrier = pltpu.get_barrier_semaphore()
    for d in range(1, T):
        pl.semaphore_signal(barrier, inc=1, device_id={"tok": lax.rem(me + d, T)}, device_id_type=pl.DeviceIdType.MESH)
    pl.semaphore_wait(barrier, T - 1)

    def tpeer(d):
        return lax.rem(me + d, T), lax.rem(me + T - d, T)

    def gpeer(d):
        a, b = lax.rem(j0 + d, G), lax.rem(j0 + G - d, G)
        return a, b, z * G + a, z * G + b

    def zpeer(d):
        a, b = lax.rem(z + d, NZ), lax.rem(z + NZ - d, NZ)
        return a, b, a * G + j0, b * G + j0

    sends = []

    def send(c):
        c.start()
        sends.append(c)

    def q_copy(t_to, t_from):
        return (remote(q_in.at[lax.rem(t_to, G)], qb.at[m128(t_from, blk)], qs.at[t_to], qr.at[t_from], t_to),
                remote(g_in.at[lax.rem(t_to, G)], gb.at[m128(t_from, blk)], gs.at[t_to], gr.at[t_from], t_to))

    def k_copy(j_to, j_from, peer):
        return (remote(k_in.at[:, m128(j_to, 128)], kb.at[m128(j_from, rows)], ks.at[j_to], kr.at[j_from], peer),
                remote(v_in.at[:, m128(j_to, 128)], vb.at[m128(j_from, rows)], vs.at[j_to], vr.at[j_from], peer))

    def x_copy(b, j_to, j_from, peer):
        return remote(x_in.at[:, m128(b * G + j_to, W)], vis.at[b, m128(j_from, rows)], xs.at[j_to, b], xr.at[j_from, b], peer)

    local = [
        pltpu.make_async_copy(q_in.at[j0], qb.at[m128(me, blk)], loc.at[0]),
        pltpu.make_async_copy(g_in.at[j0], gb.at[m128(me, blk)], loc.at[1]),
        pltpu.make_async_copy(k_in.at[:, m128(j0, 128)], kb.at[m128(j0, rows)], loc.at[2]),
        pltpu.make_async_copy(v_in.at[:, m128(j0, 128)], vb.at[m128(j0, rows)], loc.at[3]),
    ]
    local_x = [pltpu.make_async_copy(x_in.at[:, m128(b * G + j0, W)], vis.at[b, m128(j0, rows)], loc.at[4 + b]) for b in range(NV)]
    for c in local:
        c.start()
    for d in range(1, T):
        to, _ = tpeer(d)
        for c in q_copy(to, me):
            send(c)
    for d in range(1, G):
        a, _, peer, _ = gpeer(d)
        for c in k_copy(a, j0, peer):
            send(c)
    for c in local_x:
        c.start()
    for d in range(1, G):
        a, _, peer, _ = gpeer(d)
        for b in range(NV):
            send(x_copy(b, a, j0, peer))
    for c in local:
        c.wait()
    for d in range(1, G):
        _, b, _, _ = gpeer(d)
        for c in k_copy(j0, b, me):
            c.wait_recv()
    for d in range(1, T):
        _, frm = tpeer(d)
        for c in q_copy(me, frm):
            c.wait_recv()

    n_frames = NK // FR
    frame0 = z * n_frames
    stat[0:1, :] = jnp.full((1, NR), NEG_FILL, F32)
    stat[1:8, :] = jnp.zeros((7, NR), F32)

    @pl.loop(0, n_frames)
    def _(f):
        kc = kb[m128(f, FR), :]
        for r in range(0, NR, RB):
            cols = pl.ds(r, RB)
            ok = (bounds[0:1, cols] <= frame0 + f) & (frame0 + f < bounds[1:2, cols])
            s = jnp.where(ok, dot(kc, qb[cols, :], NT) * scale, NEG_FILL)
            ebuf[m128(f, FR), cols] = s
            stat[0:1, cols] = jnp.maximum(stat[0:1, cols], jnp.max(s, axis=0, keepdims=True))

    @pl.loop(0, n_frames)
    def _(f):
        vc = vb[m128(f, FR), :]
        for r in range(0, NR, RB):
            cols = pl.ds(r, RB)
            dp = dot(vc, gb[cols, :], NT)
            e = jnp.exp(ebuf[m128(f, FR), cols] - stat[0:1, cols])
            ebuf[m128(f, FR), cols] = e
            dpb[m128(f, FR), cols] = dp
            stat[1:2, cols] += jnp.sum(e, axis=0, keepdims=True)
            stat[2:3, cols] += jnp.sum(e * dp, axis=0, keepdims=True)

    def s_copy(z_to, z_from, peer):
        return remote(stat, stin.at[z_from], ss.at[z_to], sr.at[z_from], peer)

    for d in range(1, NZ):
        a, _, peer, _ = zpeer(d)
        send(s_copy(a, z, peer))
    stin[z] = stat[...]
    for d in range(1, NZ):
        _, b, _, _ = zpeer(d)
        s_copy(z, b, me).wait_recv()
    top = stat[0:1, :]
    for i in range(NZ):
        top = jnp.maximum(top, stin[i, 0:1, :])
    total = jnp.zeros((1, NR), F32)
    dotted = jnp.zeros((1, NR), F32)
    for i in range(NZ):
        w = jnp.exp(stin[i, 0:1, :] - top)
        total += w * stin[i, 1:2, :]
        dotted += w * stin[i, 2:3, :]
    coef[0:1, :] = jnp.exp(stat[0:1, :] - top) / total
    coef[1:2, :] = dotted / total
    dqt[...] = jnp.zeros_like(dqt)

    NC = cfg["NC"]
    CH = NK // NC

    def kv_copy(c, j_to, j_from, peer):
        here = kv.at[j_from, pl.ds(c * CH, CH)]
        return remote(here, here, kvs.at[j_to, c], kvr.at[j_from, c], peer)

    for c in range(NC):
        @pl.loop(c * (CH // FR), (c + 1) * (CH // FR))
        def _(f):
            kt = kb[m128(f, FR), :].astype(F32).T.astype(BF16)
            dk = jnp.zeros((FR, HEAD_WIDTH), F32)
            dv = jnp.zeros((FR, HEAD_WIDTH), F32)
            for r in range(0, NR, RB):
                cols = pl.ds(r, RB)
                p = ebuf[m128(f, FR), cols] * coef[0:1, cols]
                t = (p * (dpb[m128(f, FR), cols] - coef[1:2, cols])).astype(BF16)
                dv += dot(p.astype(BF16), gb[cols, :])
                dk += dot(t, qb[cols, :])
                dqt[:, cols] += dot(kt, t)
            kv[j0, m128(f, FR), 0:HEAD_WIDTH] = (scale * dk).astype(BF16)
            kv[j0, m128(f, FR), HEAD_WIDTH:2 * HEAD_WIDTH] = dv.astype(BF16)

        for d in range(1, G):
            a, _, peer, _ = gpeer(d)
            send(kv_copy(c, a, j0, peer))

    for r in range(0, NR, 128):
        dqs[pl.ds(r, 128), :] = (scale * dqt[:, pl.ds(r, 128)].T).astype(BF16)
    QR = NR // NZ

    def d_copy(z_to, z_from, peer):
        return remote(dqs.at[m128(z_to, QR)], dqin.at[z_from], ds.at[z_to], dr.at[z_from], peer)

    def a_copy(z_to, z_from, peer):
        here = dqall.at[j0, m128(z_from, QR)]
        return remote(here, here, as_.at[z_to], ar.at[z_from], peer)

    def y_copy(j_to, j_from, peer):
        here = dqall.at[j_from]
        return remote(here, here, ys.at[j_to], yr.at[j_from], peer)

    def r_copy(j, z_to, z_from, peer):
        return remote(part.at[j, m128(z_to, FB)], rsb.at[z_from, j], rs.at[j, z_to], rr.at[j, z_from], peer)

    for d in range(1, NZ):
        a, _, peer, _ = zpeer(d)
        send(d_copy(a, z, peer))
    for c in local_x:
        c.wait()
    for d in range(1, G):
        _, b, _, _ = gpeer(d)
        for i in range(NV):
            x_copy(i, j0, b, me).wait_recv()

    def weigh(j):
        @pl.loop(0, NV)
        def _(b):
            part[j, m128(b, W), :] = dot(vis[b], kv[j], TN).astype(BF16)
        for d in range(1, NZ):
            a, _, peer, _ = zpeer(d)
            send(r_copy(j, a, z, peer))

    weigh(j0)
    mine = dqs[m128(z, QR), :].astype(F32)
    for d in range(1, NZ):
        _, b, _, _ = zpeer(d)
        d_copy(z, b, me).wait_recv()
        mine += dqin[b].astype(F32)
    dqall[j0, m128(z, QR), :] = mine.astype(BF16)
    for d in range(1, NZ):
        a, _, peer, _ = zpeer(d)
        send(a_copy(a, z, peer))

    def spread():
        for d in range(1, NZ):
            _, b, _, _ = zpeer(d)
            a_copy(z, b, me).wait_recv()
        for d in range(1, G):
            a, _, peer, _ = gpeer(d)
            send(y_copy(a, j0, peer))

    if G == 1:
        spread()
    for d in range(1, G):
        _, b, _, _ = gpeer(d)
        for c in range(NC):
            kv_copy(c, j0, b, me).wait_recv()
        weigh(b)
        if d == 1:
            spread()
    for d in range(1, G):
        _, b, _, _ = gpeer(d)
        y_copy(j0, b, me).wait_recv()
    out_copy = pltpu.make_async_copy(dqall, q_out, loc.at[0])
    out_copy.start()

    for d in range(1, NZ):
        _, b, _, _ = zpeer(d)
        for j in range(G):
            r_copy(j, z, b, me).wait_recv()
    for j in range(G):
        acc = part[j, m128(z, FB), :].astype(F32)
        for d in range(1, NZ):
            _, b, _, _ = zpeer(d)
            acc += rsb[b, j].astype(F32)
        kw_out[:, pl.ds(j * HEAD_WIDTH, HEAD_WIDTH)] = acc[:, 0:HEAD_WIDTH]
        vw_out[:, pl.ds(j * HEAD_WIDTH, HEAD_WIDTH)] = acc[:, HEAD_WIDTH:]
    out_copy.wait()
    for c in sends:
        c.wait_send()


def shards(T, text_queries, text_grads, vision_keys, video_value_rows, vision, lengths, frame_range):
    R, QW = text_queries.shape
    rows, kv_width = vision_keys.shape
    G = kv_width // HEAD_WIDTH
    M = QW // kv_width
    NZ = T // G
    DW = vision.shape[1]
    blk, NK, NR = M * R, G * rows, T * M * R
    FB = DW // T
    W = FB if FB % 128 == 0 else 256
    NV = DW // (G * W)
    FR = rows // FRAME_DEV
    NC = 4 if NK >= 16 * FR else 1
    cfg = dict(T=T, G=G, NZ=NZ, blk=blk, rows=rows, NK=NK, NR=NR, FR=FR, W=W, NV=NV, FB=FB, NC=NC, RB=min(NR, 512))

    text_len = R * T
    row_ids = jnp.arange(text_len, dtype=jnp.int32)
    segment_ends = jnp.cumsum(lengths)
    segment = jnp.sum((row_ids[:, None] >= segment_ends[None, :]).astype(jnp.int32), axis=1)
    segment_pick = (
        segment[:, None] == jnp.arange(lengths.shape[0], dtype=jnp.int32)[None, :]
    ).astype(jnp.int32)
    bounds = jnp.sum(segment_pick[None] * frame_range.T[:, None, :], axis=2)
    bounds = jnp.broadcast_to(bounds.reshape(2, T, 1, R), (2, T, M, R)).reshape(2, NR)

    def split(a):
        return a.reshape(R, G, M, HEAD_WIDTH).transpose(1, 2, 0, 3).reshape(G, blk, HEAD_WIDTH)

    anyspec = pl.BlockSpec(memory_space=pl.ANY)
    vm = pl.BlockSpec(memory_space=pltpu.VMEM)
    V = pltpu.VMEM
    D = pltpu.SemaphoreType.DMA
    sem_pairs = []
    for shape in ((T,), (T,), (G,), (G,), (G, NV), (NZ,), (G, NC), (NZ,), (NZ,), (G,), (G, NZ)):
        sem_pairs += [D(shape), D(shape)]
    q_grad, kw, vw = pl.pallas_call(
        functools.partial(kernel, cfg),
        out_shape=(
            jax.ShapeDtypeStruct((G, NR, HEAD_WIDTH), BF16),
            jax.ShapeDtypeStruct((FB, kv_width), F32),
            jax.ShapeDtypeStruct((FB, kv_width), F32),
        ),
        in_specs=[anyspec] * 5 + [vm],
        out_specs=(anyspec, vm, vm),
        scratch_shapes=[
            V((NR, HEAD_WIDTH), BF16), V((NR, HEAD_WIDTH), BF16),
            V((NK, HEAD_WIDTH), BF16), V((NK, HEAD_WIDTH), BF16),
            V((NV, NK, W), BF16),
            V((NK, NR), F32), V((NK, NR), F32),
            V((8, NR), F32), V((NZ, 8, NR), F32), V((8, NR), F32),
            V((G, NK, 2 * HEAD_WIDTH), BF16),
            V((HEAD_WIDTH, NR), F32), V((NR, HEAD_WIDTH), BF16),
            V((NZ, NR // NZ, HEAD_WIDTH), BF16), V((G, NR, HEAD_WIDTH), BF16),
            V((G, DW // G, 2 * HEAD_WIDTH), BF16),
            V((NZ, G, FB, 2 * HEAD_WIDTH), BF16),
            D((4 + NV,)),
        ] + sem_pairs,
        compiler_params=pltpu.CompilerParams(
            collective_id=0, has_side_effects=True, vmem_limit_bytes=67043328
        ),
    )(split(text_queries), split(text_grads), vision_keys, video_value_rows, vision, bounds)
    q_grad = q_grad.reshape(G, T, M, R, HEAD_WIDTH).transpose(1, 3, 0, 2, 4).reshape(text_len, QW)
    return q_grad, kw, vw


def solution(mesh):
    return jax.shard_map(
        functools.partial(shards, mesh.shape["tok"]),
        mesh=mesh,
        in_specs=(
            P("tok", "head"),
            P("tok", "head"),
            P("tok", "head"),
            P("tok", "head"),
            P("tok", None),
            P(),
            P(),
        ),
        out_specs=(P(None, "head"), P("tok", "head"), P("tok", "head")),
        check_vma=False,
    )
```

```python
import functools

import jax
import jax.numpy as jnp
from jax import lax
from jax.experimental import pallas as pl
from jax.experimental.pallas import tpu as pltpu
from jax.sharding import PartitionSpec as P

HEAD_WIDTH = 128
FRAME_DEV = 4
NEG_FILL = -1e30
NT = (((1,), (1,)), ((), ()))
TN = (((0,), (0,)), ((), ()))
F32 = jnp.float32
BF16 = jnp.bfloat16


def dot(a, b, dims=(((1,), (0,)), ((), ()))):
    return lax.dot_general(a, b, dims, preferred_element_type=F32)


def kernel(cfg, q_in, g_in, k_in, v_in, x_in, bounds, q_out, kw_out, vw_out,
           qb, gb, kb, vb, vis, ebuf, dpb, stat, stin, coef, kv, dqt, dqs, dqin, dqall, part, rsb,
           loc, qs, qr, gs, gr, ks, kr, vs, vr, xs, xr, ss, sr, kvs, kvr, ds, dr, as_, ar, ys, yr, rs, rr, fs, fr):
    T, G, NZ = cfg["T"], cfg["G"], cfg["NZ"]
    blk, rows, NK, NR, FR = cfg["blk"], cfg["rows"], cfg["NK"], cfg["NR"], cfg["FR"]
    W, NV, FB = cfg["W"], cfg["NV"], cfg["FB"]
    H = cfg["H"]
    RB = cfg["RB"]
    scale = HEAD_WIDTH ** (-0.5)
    me = lax.axis_index("tok")
    z, j0 = me // G, me % G

    def remote(src, dst, s, r, peer):
        return pltpu.make_async_remote_copy(
            src_ref=src, dst_ref=dst, send_sem=s, recv_sem=r,
            device_id={"tok": peer}, device_id_type=pl.DeviceIdType.MESH)

    def m128(i, n):
        return pl.ds(pl.multiple_of(i * n, n), n)

    barrier = pltpu.get_barrier_semaphore()
    for d in range(1, T):
        pl.semaphore_signal(barrier, inc=1, device_id={"tok": lax.rem(me + d, T)}, device_id_type=pl.DeviceIdType.MESH)
    twin = lax.axis_index("head")
    if H > 1:
        twin = 1 - twin
        pl.semaphore_signal(barrier, inc=1, device_id={"head": twin}, device_id_type=pl.DeviceIdType.MESH)
    pl.semaphore_wait(barrier, T - 1 + (H > 1))

    def tpeer(d):
        return lax.rem(me + d, T), lax.rem(me + T - d, T)

    def gpeer(d):
        a, b = (j0 ^ d, j0 ^ d) if G & (G - 1) == 0 else (lax.rem(j0 + d, G), lax.rem(j0 + G - d, G))
        return a, b, z * G + a, z * G + b

    def zpeer(d):
        a, b = lax.rem(z + d, NZ), lax.rem(z + NZ - d, NZ)
        return a, b, a * G + j0, b * G + j0

    sends = []

    def send(c):
        c.start()
        sends.append(c)

    def q_copy(t_to, t_from):
        return (remote(q_in.at[lax.rem(t_to, G)], qb.at[m128(t_from, blk)], qs.at[t_to], qr.at[t_from], t_to),
                remote(g_in.at[lax.rem(t_to, G)], gb.at[m128(t_from, blk)], gs.at[t_to], gr.at[t_from], t_to))

    def k_copy(j_to, j_from, peer):
        return (remote(k_in.at[:, m128(j_to, 128)], kb.at[m128(j_from, rows)], ks.at[j_to], kr.at[j_from], peer),
                remote(v_in.at[:, m128(j_to, 128)], vb.at[m128(j_from, rows)], vs.at[j_to], vr.at[j_from], peer))

    WH = W // H
    half = lax.axis_index("head") * WH if H > 1 else 0

    def x_copy(b, j_to, j_from, peer):
        cols = pl.ds(pl.multiple_of((b * G + j_to) * W + half, WH), WH)
        dst = vis.at[b, m128(j_from, rows), pl.ds(pl.multiple_of(half, WH), WH)]
        return remote(x_in.at[:, cols], dst, xs.at[j_to, b], xr.at[j_from, b], peer)

    def f_copy(b, j_from, mine):
        at = half if mine else WH - half
        here = vis.at[b, m128(j_from, rows), pl.ds(pl.multiple_of(at, WH), WH)]
        return pltpu.make_async_remote_copy(
            src_ref=here, dst_ref=here, send_sem=fs.at[j_from, b], recv_sem=fr.at[j_from, b],
            device_id={"head": twin}, device_id_type=pl.DeviceIdType.MESH)

    local = [
        pltpu.make_async_copy(q_in.at[j0], qb.at[m128(me, blk)], loc.at[0]),
        pltpu.make_async_copy(g_in.at[j0], gb.at[m128(me, blk)], loc.at[1]),
        pltpu.make_async_copy(k_in.at[:, m128(j0, 128)], kb.at[m128(j0, rows)], loc.at[2]),
        pltpu.make_async_copy(v_in.at[:, m128(j0, 128)], vb.at[m128(j0, rows)], loc.at[3]),
    ]
    local_x = [pltpu.make_async_copy(x_in.at[:, m128(b * G + j0, W)], vis.at[b, m128(j0, rows)], loc.at[4 + b]) for b in range(NV)]
    for c in local:
        c.start()
    def q_sends(zd):
        a, _, _, _ = zpeer(zd)
        for i in range(G):
            to = a * G + (lax.rem(j0 + i, G) if zd else gpeer(i)[0])
            if zd or i:
                for c in q_copy(to, me):
                    send(c)

    q_sends(0)
    for d in range(1, G):
        a, _, peer, _ = gpeer(d)
        for c in k_copy(a, j0, peer):
            send(c)
    for d in range(1, NZ):
        q_sends(d)
    for c in local_x:
        c.start()
    for c in local:
        c.wait()
    for d in range(1, G):
        _, b, _, _ = gpeer(d)
        for c in k_copy(j0, b, me):
            c.wait_recv()

    def q_wait(zd):
        _, b, _, _ = zpeer(zd)
        for i in range(G):
            if zd or i:
                frm = b * G + (i if zd else gpeer(i)[1])
                for c in q_copy(me, frm):
                    c.wait_recv()

    n_frames = NK // FR
    frame0 = z * n_frames
    stat[0:1, :] = jnp.full((1, NR), NEG_FILL, F32)
    stat[1:8, :] = jnp.zeros((7, NR), F32)

    def totals(cols, width):
        first, end = bounds[0:1, cols], bounds[1:2, cols]
        UN = 2 if n_frames % 2 == 0 else 1

        def scored(i, top):
            for u in range(UN):
                f = i * UN + u
                ok = (first <= frame0 + f) & (frame0 + f < end)
                s = jnp.where(ok, dot(kb[m128(f, FR), :], qb[cols, :], NT) * scale, NEG_FILL)
                ebuf[m128(f, FR), cols] = s
                top = jnp.maximum(top, jnp.max(s, axis=0, keepdims=True))
            return top

        top = lax.fori_loop(0, n_frames // UN, scored, jnp.full((1, width), NEG_FILL, F32))

        def summed(i, carry):
            total, dotted = carry
            for u in range(UN):
                f = i * UN + u
                dp = dot(vb[m128(f, FR), :], gb[cols, :], NT)
                e = jnp.exp(ebuf[m128(f, FR), cols] - top)
                ebuf[m128(f, FR), cols] = e
                dpb[m128(f, FR), cols] = dp
                total += jnp.sum(e, axis=0, keepdims=True)
                dotted += jnp.sum(e * dp, axis=0, keepdims=True)
            return total, dotted

        zero = jnp.zeros((1, width), F32)
        total, dotted = lax.fori_loop(0, n_frames // UN, summed, (zero, zero))
        stat[0:1, cols] = top
        stat[1:2, cols] = total
        stat[2:3, cols] = dotted

    def x_sends():
        for d in range(1, G):
            a, _, peer, _ = gpeer(d)
            for b in range(NV):
                send(x_copy(b, a, j0, peer))

    by_z = (NR // NZ) % 128 == 0
    for d in range(NZ):
        q_wait(d)
        if d == NZ - 1:
            x_sends()
        if by_z:
            totals(m128(zpeer(d)[1], NR // NZ), NR // NZ)
    if not by_z:
        for r in range(0, NR, RB):
            totals(pl.ds(r, RB), RB)

    def s_copy(z_to, z_from, peer):
        return remote(stat, stin.at[z_from], ss.at[z_to], sr.at[z_from], peer)

    for d in range(1, NZ):
        a, _, peer, _ = zpeer(d)
        send(s_copy(a, z, peer))
    stin[z] = stat[...]
    for d in range(1, NZ):
        _, b, _, _ = zpeer(d)
        s_copy(z, b, me).wait_recv()
    top = stat[0:1, :]
    for i in range(NZ):
        top = jnp.maximum(top, stin[i, 0:1, :])
    total = jnp.zeros((1, NR), F32)
    dotted = jnp.zeros((1, NR), F32)
    for i in range(NZ):
        w = jnp.exp(stin[i, 0:1, :] - top)
        total += w * stin[i, 1:2, :]
        dotted += w * stin[i, 2:3, :]
    coef[0:1, :] = jnp.exp(stat[0:1, :] - top) / total
    coef[1:2, :] = dotted / total
    dqt[...] = jnp.zeros_like(dqt)

    NC = cfg["NC"]
    CH = NK // NC

    def kv_copy(c, j_to, j_from, peer):
        here = kv.at[j_from, pl.ds(c * CH, CH)]
        return remote(here, here, kvs.at[j_to, c], kvr.at[j_from, c], peer)

    for c in range(NC):
        @pl.loop(c * (CH // FR), (c + 1) * (CH // FR))
        def _(f):
            kt = kb[m128(f, FR), :].astype(F32).T.astype(BF16)
            dk = jnp.zeros((FR, HEAD_WIDTH), F32)
            dv = jnp.zeros((FR, HEAD_WIDTH), F32)
            for r in range(0, NR, RB):
                cols = pl.ds(r, RB)
                p = ebuf[m128(f, FR), cols] * coef[0:1, cols]
                t = (p * (dpb[m128(f, FR), cols] - coef[1:2, cols])).astype(BF16)
                dv += dot(p.astype(BF16), gb[cols, :])
                dk += dot(t, qb[cols, :])
                dqt[:, cols] += dot(kt, t)
            kv[j0, m128(f, FR), 0:HEAD_WIDTH] = (scale * dk).astype(BF16)
            kv[j0, m128(f, FR), HEAD_WIDTH:2 * HEAD_WIDTH] = dv.astype(BF16)

        for d in range(1, G - 1):
            a, _, peer, _ = gpeer(d)
            kv_copy(c, a, j0, peer).start()
        if H > 1 and c == NC // 2:
            for d in range(1, G):
                _, b, _, _ = gpeer(d)
                for i in range(NV):
                    x_copy(i, j0, b, me).wait_recv()
                    send(f_copy(i, b, True))

    for r in range(0, NR, 128):
        dqs[pl.ds(r, 128), :] = (scale * dqt[:, pl.ds(r, 128)].T).astype(BF16)
    QR = NR // NZ

    def d_copy(z_to, z_from, peer):
        return remote(dqs.at[m128(z_to, QR)], dqin.at[z_from], ds.at[z_to], dr.at[z_from], peer)

    def a_copy(z_to, z_from, peer):
        here = dqall.at[j0, m128(z_from, QR)]
        return remote(here, here, as_.at[z_to], ar.at[z_from], peer)

    def y_copy(j_to, j_from, peer):
        here = dqall.at[j_from]
        return remote(here, here, ys.at[j_to], yr.at[j_from], peer)

    def r_copy(j, z_to, z_from, peer):
        return remote(part.at[j, m128(z_to, FB)], rsb.at[z_from, j], rs.at[j, z_to], rr.at[j, z_from], peer)

    for d in range(1, NZ):
        a, _, peer, _ = zpeer(d)
        send(d_copy(a, z, peer))
    for c in local_x:
        c.wait()
    for d in range(1, G):
        _, b, _, _ = gpeer(d)
        for i in range(NV):
            (f_copy(i, b, False) if H > 1 else x_copy(i, j0, b, me)).wait_recv()

    def weigh(j):
        @pl.loop(0, NV)
        def _(b):
            part[j, m128(b, W), :] = dot(vis[b], kv[j], TN).astype(BF16)
        for d in range(1, NZ):
            a, _, peer, _ = zpeer(d)
            send(r_copy(j, a, z, peer))

    weigh(j0)
    mine = dqs[m128(z, QR), :].astype(F32)
    for d in range(1, NZ):
        _, b, _, _ = zpeer(d)
        d_copy(z, b, me).wait_recv()
        mine += dqin[b].astype(F32)
    dqall[j0, m128(z, QR), :] = mine.astype(BF16)
    for d in range(1, NZ):
        a, _, peer, _ = zpeer(d)
        send(a_copy(a, z, peer))

    def spread():
        for d in range(1, NZ):
            _, b, _, _ = zpeer(d)
            a_copy(z, b, me).wait_recv()
        for d in range(1, G):
            a, _, peer, _ = gpeer(d)
            send(y_copy(a, j0, peer))

    for d in range(1, G - 1):
        a, _, peer, _ = gpeer(d)
        for c in range(NC):
            kv_copy(c, a, j0, peer).wait_send()
    if G > 1:
        a, _, peer, _ = gpeer(G - 1)
        for c in range(NC):
            send(kv_copy(c, a, j0, peer))
    if G == 1:
        spread()
    for d in range(1, G):
        _, b, _, _ = gpeer(d)
        for c in range(NC):
            kv_copy(c, j0, b, me).wait_recv()
        weigh(b)
        if d == min(2, G - 1):
            spread()
    for d in range(1, G):
        _, b, _, _ = gpeer(d)
        y_copy(j0, b, me).wait_recv()
    out_copy = pltpu.make_async_copy(dqall, q_out, loc.at[0])
    out_copy.start()

    for d in range(1, NZ):
        _, b, _, _ = zpeer(d)
        for j in range(G):
            r_copy(j, z, b, me).wait_recv()
    for j in range(G):
        acc = part[j, m128(z, FB), :].astype(F32)
        for d in range(1, NZ):
            _, b, _, _ = zpeer(d)
            acc += rsb[b, j].astype(F32)
        kw_out[:, pl.ds(j * HEAD_WIDTH, HEAD_WIDTH)] = acc[:, 0:HEAD_WIDTH]
        vw_out[:, pl.ds(j * HEAD_WIDTH, HEAD_WIDTH)] = acc[:, HEAD_WIDTH:]
    out_copy.wait()
    for c in sends:
        c.wait_send()


def shards(T, cores, text_queries, text_grads, vision_keys, video_value_rows, vision, lengths, frame_range):
    R, QW = text_queries.shape
    rows, kv_width = vision_keys.shape
    G = kv_width // HEAD_WIDTH
    M = QW // kv_width
    NZ = T // G
    DW = vision.shape[1]
    blk, NK, NR = M * R, G * rows, T * M * R
    FB = DW // T
    W = FB if FB % 128 == 0 else 256
    NV = DW // (G * W)
    FR = rows // FRAME_DEV
    NC = 4 if NK >= 16 * FR else 1
    cfg = dict(T=T, G=G, NZ=NZ, blk=blk, rows=rows, NK=NK, NR=NR, FR=FR, W=W, NV=NV, FB=FB, NC=NC, RB=min(NR, 512),
               H=2 if cores == 2 and G > 1 and W % 256 == 0 else 1)

    text_len = R * T
    row_ids = jnp.arange(text_len, dtype=jnp.int32)
    segment_ends = jnp.cumsum(lengths)
    segment = jnp.sum((row_ids[:, None] >= segment_ends[None, :]).astype(jnp.int32), axis=1)
    segment_pick = (
        segment[:, None] == jnp.arange(lengths.shape[0], dtype=jnp.int32)[None, :]
    ).astype(jnp.int32)
    bounds = jnp.sum(segment_pick[None] * frame_range.T[:, None, :], axis=2)
    bounds = jnp.broadcast_to(bounds.reshape(2, T, 1, R), (2, T, M, R)).reshape(2, NR)

    def split(a):
        return a.reshape(R, G, M, HEAD_WIDTH).transpose(1, 2, 0, 3).reshape(G, blk, HEAD_WIDTH)

    anyspec = pl.BlockSpec(memory_space=pl.ANY)
    vm = pl.BlockSpec(memory_space=pltpu.VMEM)
    V = pltpu.VMEM
    D = pltpu.SemaphoreType.DMA
    sem_pairs = []
    for shape in ((T,), (T,), (G,), (G,), (G, NV), (NZ,), (G, NC), (NZ,), (NZ,), (G,), (G, NZ), (G, NV)):
        sem_pairs += [D(shape), D(shape)]
    q_grad, kw, vw = pl.pallas_call(
        functools.partial(kernel, cfg),
        out_shape=(
            jax.ShapeDtypeStruct((G, NR, HEAD_WIDTH), BF16),
            jax.ShapeDtypeStruct((FB, kv_width), F32),
            jax.ShapeDtypeStruct((FB, kv_width), F32),
        ),
        in_specs=[anyspec] * 5 + [vm],
        out_specs=(anyspec, vm, vm),
        scratch_shapes=[
            V((NR, HEAD_WIDTH), BF16), V((NR, HEAD_WIDTH), BF16),
            V((NK, HEAD_WIDTH), BF16), V((NK, HEAD_WIDTH), BF16),
            V((NV, NK, W), BF16),
            V((NK, NR), F32), V((NK, NR), F32),
            V((8, NR), F32), V((NZ, 8, NR), F32), V((8, NR), F32),
            V((G, NK, 2 * HEAD_WIDTH), BF16),
            V((HEAD_WIDTH, NR), F32), V((NR, HEAD_WIDTH), BF16),
            V((NZ, NR // NZ, HEAD_WIDTH), BF16), V((G, NR, HEAD_WIDTH), BF16),
            V((G, DW // G, 2 * HEAD_WIDTH), BF16),
            V((NZ, G, FB, 2 * HEAD_WIDTH), BF16),
            D((4 + NV,)),
        ] + sem_pairs,
        compiler_params=pltpu.CompilerParams(
            collective_id=0, has_side_effects=True, vmem_limit_bytes=67043328
        ),
    )(split(text_queries), split(text_grads), vision_keys, video_value_rows, vision, bounds)
    q_grad = q_grad.reshape(G, T, M, R, HEAD_WIDTH).transpose(1, 3, 0, 2, 4).reshape(text_len, QW)
    return q_grad, kw, vw


def solution(mesh):
    return jax.shard_map(
        functools.partial(shards, mesh.shape["tok"], mesh.shape["head"]),
        mesh=mesh,
        in_specs=(
            P("tok", "head"),
            P("tok", "head"),
            P("tok", "head"),
            P("tok", "head"),
            P("tok", None),
            P(),
            P(),
        ),
        out_specs=(P(None, "head"), P("tok", "head"), P("tok", "head")),
        check_vma=False,
    )
```
